32 devices in a mesh: atoms: 8 (over z, y), modes: 4 (over x, core).
Axes of the slice: x: 2, y: 2, z: 4, core: 2. Of those that a mesh axis runs over, the one named last changes fastest.
Arguments:
- eigvec: bfloat16 [3072, 2048], P('atoms', 'modes'), may hold values from -6 to 6
- operator_blocks: bfloat16 [24, 8, 128, 128], P('atoms'), may hold values from -0.0034179688 to 0.0034179688
- column_blocks: int32 [24, 8], P('atoms'), may hold values from 0 to 23, as said below
- block_mask: int32 [24, 8], P('atoms'), may hold values 0 or 1
- spectrum: float32 [3072], replicated, may hold values from 0.5 to 20
- mode_index: int32 [2048], replicated, may hold values from 0 to 3071
- linewidth: float32 [2048], replicated, may hold values from 0.05 to 1
Outputs:
- flux_tiles: float32 [2048, 2048], P('modes', 'atoms')
- diffusivity: float32 [2048], P('modes')
The draws below stay inside these ranges and needn't reach their ends.
Inputs may be any that keep to these rules, and one draw needn't show every extreme that they name: `column_blocks`: the 8 column blocks of row block r are distinct and lie within 4 blocks of r, counted around the cycle of 24 blocks.
All inputs are finite; a program needn't handle non-finite values. No bound on the sum of `block_mask` on one device may be relied on, other than what follows from the above.
Results may differ from the reference program's by a relative error of at most 0.0058.
Values may be sent and summed in bfloat16 or wider, within the bound.
No kernel may reach another device: no remote copies, remote signals or barrier semaphores. Data moves between devices by JAX's collectives and lax.ppermute only.
A program may use at most 64 MiB of HBM per device.

```python
import math
import jax
import jax.numpy as jnp
from jax import lax

BS = 128
SLOTS = 8
REACH = 4
M = 2048
NB = 24
COORDS = 3072


def draw_column_blocks(key, part):
    candidates = 2 * REACH + 1
    random_bits = jax.random.randint(key, (NB, candidates), 0, 2 ** 20)
    scores = random_bits * candidates + jnp.arange(candidates, dtype=jnp.int32)[None, :]
    chosen = jnp.argsort(scores, axis=1)[:, :SLOTS].astype(jnp.int32)
    row_blocks = jnp.arange(NB, dtype=jnp.int32)[:, None]
    return ((row_blocks + chosen - REACH) % NB).astype(jnp.int32)


def touch_ends(array, stream_key, smallest, largest):
    spot = [jax.random.randint(jax.random.fold_in(stream_key, axis), (), 0, length) for axis, length in enumerate(array.shape)]
    widest = array.shape.index(max(array.shape))
    next_to = spot[:widest] + [(spot[widest] + 1) % array.shape[widest]] + spot[widest + 1:]
    return array.at[tuple(spot)].set(smallest).at[tuple(next_to)].set(largest)


def shard_levels(own_key, shape, shards, least, high):
    factor_of, own = 1.0, jax.random.fold_in(own_key, 6)
    for axis_at, shards_of in shards:
        steps = jnp.exp(jax.random.uniform(jax.random.fold_in(own, axis_at), (shards_of,), jnp.float32, least / len(shards), high / len(shards)))
        factor_of = factor_of * jnp.repeat(steps, shape[axis_at] // shards_of).reshape([-1 if axis == axis_at else 1 for axis in range(len(shape))])
    return factor_of


def noise(rng, shape, width, most, shards=(), kind=jnp.bfloat16):
    values = width * jax.random.normal(rng, shape, jnp.float32)
    if shards:
        values = values * shard_levels(rng, shape, shards, -0.22, 0.18)
    return jnp.clip(values, -most, most).astype(kind)


def setup_inputs(seed: int = 0) -> dict:
    splits = jax.random.split(jax.random.key(seed), 8)
    eigvec = noise(splits[0], (COORDS, M), 1.0, 6.0, ((0, 8), (1, 4)))
    operator_blocks = noise(splits[1], (NB, SLOTS, BS, BS), (SLOTS * BS * COORDS) ** -0.5, 0.0034179688, ((0, 8),))
    column_blocks = draw_column_blocks(jax.random.fold_in(splits[7], 71), 0)
    block_mask = touch_ends((jax.random.randint(splits[3], (NB, SLOTS), 0, 4) < 3).astype(jnp.int32), jax.random.fold_in(splits[3], 1), 0, 1)
    spectrum = jnp.clip(jnp.exp(jax.random.uniform(splits[4], (COORDS,), jnp.float32, math.log(0.5), math.log(20.0))), 0.5, 20.0)
    mode_index = touch_ends(jax.random.randint(splits[5], (M,), 0, COORDS), jax.random.fold_in(splits[5], 1), 0, COORDS - 1).astype(jnp.int32)
    linewidth = jnp.clip(jnp.exp(jax.random.uniform(splits[6], (M,), jnp.float32, math.log(0.05), math.log(1.0))), 0.05, 1.0)
    return dict(eigvec=eigvec, operator_blocks=operator_blocks, column_blocks=column_blocks, block_mask=block_mask, spectrum=spectrum, mode_index=mode_index, linewidth=linewidth)


def pair_weight(row_freq, col_freq, row_width, col_width):
    freq_sum = row_freq[:, None] + col_freq[None, :]
    spacing = row_freq[:, None] - col_freq[None, :]
    mean_width = 0.5 * (row_width[:, None] + col_width[None, :])
    factor = freq_sum * freq_sum / (4.0 * row_freq[:, None] * col_freq[None, :])
    return factor * mean_width / (spacing * spacing + mean_width * mean_width)


def reference(eigvec, operator_blocks, column_blocks, block_mask, spectrum, mode_index, linewidth):
    eig_blocks = eigvec.reshape(NB, BS, M)
    masked = jnp.where(block_mask[:, :, None, None] > 0, operator_blocks, jnp.zeros((), operator_blocks.dtype))
    product = jnp.zeros((NB, BS, M), jnp.float32)
    for slot_index in range(SLOTS):
        picked = eig_blocks[column_blocks[:, slot_index]]
        product = product + jnp.einsum("bij,bjm->bim", masked[:, slot_index].astype(jnp.float32), picked.astype(jnp.float32), precision=lax.Precision.HIGHEST)
    velocity = product.reshape(COORDS, M).astype(jnp.bfloat16)
    eig_float = eigvec.astype(jnp.float32)
    vel_float = velocity.astype(jnp.float32)
    pair_sum = jnp.dot(eig_float.T, vel_float, precision=lax.Precision.HIGHEST)
    flux_tiles = pair_sum - pair_sum.T
    frequency = spectrum[mode_index]
    weight = pair_weight(frequency, frequency, linewidth, linewidth)
    diffusivity = jnp.sum(weight * flux_tiles * flux_tiles, axis=1) / M
    return flux_tiles, diffusivity
```

```python
import jax
import jax.numpy as jnp
from jax import lax
from jax.sharding import PartitionSpec as P

REACH = 4


def shifted(value, axis, by):
    count = lax.axis_size(axis)
    return lax.ppermute(value, axis, [(i, (i + by) % count) for i in range(count)])


def swapped(value, axis, bit):
    count = lax.axis_size(axis)
    return lax.ppermute(value, axis, [(i, i ^ bit) for i in range(count)])


def swapped_both(value, atom_bit, mode_bit):
    atoms, modes = lax.axis_size("atoms"), lax.axis_size("modes")
    pairs = [
        (a * modes + m, (a ^ atom_bit) * modes + (m ^ mode_bit))
        for a in range(atoms)
        for m in range(modes)
    ]
    return lax.ppermute(value, ("atoms", "modes"), pairs)


def parity_columns(value, parity, share):
    rows, cols = value.shape
    groups = cols // (2 * share)
    if groups == 1:
        return lax.dynamic_slice_in_dim(value, parity * share, share, axis=1)
    split = value.reshape(rows, groups, 2, share)
    return lax.dynamic_index_in_dim(split, parity, 2, keepdims=False).reshape(rows, groups * share)


def looked_up(table, index):
    hit = index[:, None] == jnp.arange(table.shape[0], dtype=index.dtype)[None, :]
    return jnp.sum(jnp.where(hit, table[None, :], 0.0), axis=1)


def pair_weight(row_freq, col_freq, row_width, col_width):
    freq_sum = row_freq[:, None] + col_freq[None, :]
    spacing = row_freq[:, None] - col_freq[None, :]
    mean_width = 0.5 * (row_width[:, None] + col_width[None, :])
    factor = freq_sum * freq_sum / (4.0 * row_freq[:, None] * col_freq[None, :])
    return factor * mean_width / (spacing * spacing + mean_width * mean_width)


def body(eigvec, operator_blocks, column_blocks, block_mask, spectrum, mode_index, linewidth):
    block_width = operator_blocks.shape[2]
    local_blocks = operator_blocks.shape[0]
    slab_rows, own_modes = eigvec.shape
    atom_count = lax.axis_size("atoms")
    mode_count = lax.axis_size("modes")
    atom_rank = lax.axis_index("atoms")
    mode_rank = lax.axis_index("modes")
    total_blocks = local_blocks * atom_count
    mode_total = own_modes * mode_count
    share = mode_total // atom_count
    levels = atom_count // 2
    parity = atom_rank % 2
    level = atom_rank // 2
    extra_rows = (REACH - local_blocks) * block_width

    low = shifted(eigvec, "atoms", 1)
    high = shifted(eigvec, "atoms", -1)
    far_low = shifted(eigvec[slab_rows - extra_rows :], "atoms", 2)
    far_high = shifted(eigvec[:extra_rows], "atoms", -2)
    eig_half = parity_columns(eigvec, parity, share)
    eig_half_x = swapped(eig_half, "modes", 2)

    extended = jnp.concatenate([far_low, low, eigvec, high, far_high], axis=0)
    ext_blocks = extended.reshape(-1, block_width, own_modes)
    offsets = (column_blocks - atom_rank * local_blocks + REACH) % total_blocks
    picked = ext_blocks[offsets]
    masked = jnp.where(
        block_mask[:, :, None, None] > 0, operator_blocks, jnp.zeros((), operator_blocks.dtype)
    )
    product = jnp.einsum("bsij,bsjm->bim", masked, picked, preferred_element_type=jnp.float32)
    velocity = product.reshape(-1, own_modes).astype(jnp.bfloat16)

    eig_other = jnp.where(parity == 0, high, low)
    eig_other_half = parity_columns(eig_other, parity, share)
    vel_half = parity_columns(velocity, parity, share)
    vel_away = parity_columns(velocity, 1 - parity, share)
    vel_other = swapped(velocity, "atoms", 1)
    mixed_x = swapped(jnp.concatenate([eig_other_half, vel_half], axis=0), "modes", 2)
    vel_other_half_x = swapped_both(vel_away, 1, 2)
    vel_other_half = parity_columns(vel_other, parity, share)

    mine = jnp.concatenate([vel_half, vel_other_half, -eig_half, -eig_other_half], axis=0)
    beyond = jnp.concatenate(
        [mixed_x[slab_rows:], vel_other_half_x, -eig_half_x, -mixed_x[:slab_rows]], axis=0
    )
    both = jnp.stack([mine, beyond])
    both_core = swapped(both, "modes", 1)
    left = jnp.concatenate([eigvec, eig_other, velocity, vel_other], axis=0)
    contract = (((0,), (0,)), ((), ()))
    tiles = jnp.stack(
        [
            lax.dot_general(left, right, contract, preferred_element_type=jnp.float32)
            for right in (both[0], both_core[0], both[1], both_core[1])
        ]
    )
    groups = own_modes // (2 * share)

    def tile_for(target):
        nearness = (target // groups) ^ mode_rank
        return lax.dynamic_slice(
            tiles, (nearness, 0, (target % groups) * share), (1, own_modes, share)
        )[0]

    flux_tiles = tile_for(level)
    for step in sorted(range(1, levels), key=lambda s: (s != 2, s)):
        piece = tile_for(level ^ step).astype(jnp.bfloat16)
        flux_tiles = flux_tiles + swapped(piece, "atoms", 2 * step).astype(jnp.float32)

    row_index = lax.dynamic_slice_in_dim(mode_index, mode_rank * own_modes, own_modes)
    col_index = lax.dynamic_slice_in_dim(mode_index, atom_rank * share, share)
    row_freq = looked_up(spectrum, row_index)
    col_freq = looked_up(spectrum, col_index)
    row_width = lax.dynamic_slice_in_dim(linewidth, mode_rank * own_modes, own_modes)
    col_width = lax.dynamic_slice_in_dim(linewidth, atom_rank * share, share)
    weight = pair_weight(row_freq, col_freq, row_width, col_width)
    sums = jnp.sum(weight * flux_tiles * flux_tiles, axis=1)
    bit = 1
    while bit < atom_count:
        sums = sums + swapped(sums, "atoms", bit)
        bit *= 2
    return (flux_tiles, sums / mode_total)


def solution(mesh):
    return jax.shard_map(
        body,
        mesh=mesh,
        in_specs=(
            P("atoms", "modes"),
            P("atoms", None, None, None),
            P("atoms", None),
            P("atoms", None),
            P(),
            P(),
            P(),
        ),
        out_specs=(P("modes", "atoms"), P("modes")),
        check_vma=False,
    )
```

```python
import jax
import jax.numpy as jnp
from jax import lax
from jax.experimental import pallas as pl
from jax.experimental.pallas import tpu as pltpu
from jax.sharding import PartitionSpec as P

REACH = 4


def shifted(value, axis, by):
    count = lax.axis_size(axis)
    return lax.ppermute(value, axis, [(i, (i + by) % count) for i in range(count)])


def swapped(value, axis, bit):
    count = lax.axis_size(axis)
    return lax.ppermute(value, axis, [(i, i ^ bit) for i in range(count)])


def swapped_both(value, atom_bit, mode_bit):
    atoms, modes = lax.axis_size("atoms"), lax.axis_size("modes")
    pairs = [
        (a * modes + m, (a ^ atom_bit) * modes + (m ^ mode_bit))
        for a in range(atoms)
        for m in range(modes)
    ]
    return lax.ppermute(value, ("atoms", "modes"), pairs)


def parity_columns(value, parity, share):
    rows, cols = value.shape
    groups = cols // (2 * share)
    if groups == 1:
        return lax.dynamic_slice_in_dim(value, parity * share, share, axis=1)
    split = value.reshape(rows, groups, 2, share)
    return lax.dynamic_index_in_dim(split, parity, 2, keepdims=False).reshape(rows, groups * share)


def looked_up(table, index):
    hit = index[:, None] == jnp.arange(table.shape[0], dtype=index.dtype)[None, :]
    return jnp.sum(jnp.where(hit, table[None, :], 0.0), axis=1)


def pair_weight(row_freq, col_freq, row_width, col_width):
    freq_sum = row_freq[:, None] + col_freq[None, :]
    spacing = row_freq[:, None] - col_freq[None, :]
    mean_width = 0.5 * (row_width[:, None] + col_width[None, :])
    factor = freq_sum * freq_sum / (4.0 * row_freq[:, None] * col_freq[None, :])
    return factor * mean_width / (spacing * spacing + mean_width * mean_width)


def velocity_kernel(local_blocks, slots, block_width, share, split):
    slab_rows = local_blocks * block_width
    base = REACH * block_width

    def kernel(offset, keep, parity, far_low, low, own, high, far_high, blocks, *rest):
        if split:
            velocity, other, away, mixed, ext, picked, masked = rest
        else:
            velocity, other, ext, picked, masked = rest
        row = 0
        for piece in (far_low, low, own, high, far_high):
            if piece is not None:
                ext[row : row + piece.shape[0], :] = piece[...]
                row += piece.shape[0]
        for b in range(local_blocks):
            for s in range(slots):
                here = slice(s * block_width, (s + 1) * block_width)
                source = pl.multiple_of(offset[b, s] * block_width, block_width)
                picked[here, :] = ext[pl.ds(source, block_width), :]
                block = blocks[b, s]
                masked[:, here] = jnp.where(keep[b, s] > 0, block, jnp.zeros_like(block))
            product = jnp.dot(masked[...], picked[...], preferred_element_type=jnp.float32)
            velocity[b * block_width : (b + 1) * block_width, :] = product.astype(jnp.bfloat16)
        even = parity[0] == 0
        shift = jnp.where(even, base + slab_rows, base - slab_rows)
        other_rows = ext[pl.ds(pl.multiple_of(shift, block_width), slab_rows), :]
        other[...] = other_rows
        if split:
            mixed[:slab_rows, :] = jnp.where(even, other_rows[:, :share], other_rows[:, share:])
            left, right = velocity[:, :share], velocity[:, share:]
            mixed[slab_rows:, :] = jnp.where(even, left, right)
            away[...] = jnp.where(even, right, left)

    return kernel


def tile_kernel(count):
    def kernel(pick, left_eig, left_eig_other, left_vel, left_vel_other, *rest):
        sources, (out, chosen) = rest[: 4 * count], rest[4 * count :]
        depth = left_eig.shape[1]
        for index in range(count):

            @pl.when(pick[0] == index)
            def _(index=index):
                for part in range(4):
                    chosen[part * depth : (part + 1) * depth, :] = sources[4 * index + part][...]

        plus = jnp.dot(left_eig[...], chosen[2 * depth : 3 * depth, :], preferred_element_type=jnp.float32)
        plus += jnp.dot(left_eig_other[...], chosen[3 * depth :, :], preferred_element_type=jnp.float32)
        minus = jnp.dot(left_vel[...], chosen[:depth, :], preferred_element_type=jnp.float32)
        minus += jnp.dot(left_vel_other[...], chosen[depth : 2 * depth, :], preferred_element_type=jnp.float32)
        out[...] = (plus - minus).astype(out.dtype)

    return kernel


def in_vmem():
    return pl.BlockSpec(memory_space=pltpu.VMEM)


def in_smem():
    return pl.BlockSpec(memory_space=pltpu.SMEM)


def body(eigvec, operator_blocks, column_blocks, block_mask, spectrum, mode_index, linewidth):
    local_blocks, slots, block_width, _ = operator_blocks.shape
    slab_rows, own_modes = eigvec.shape
    atom_count = lax.axis_size("atoms")
    mode_count = lax.axis_size("modes")
    atom_rank = lax.axis_index("atoms")
    mode_rank = lax.axis_index("modes")
    total_blocks = local_blocks * atom_count
    mode_total = own_modes * mode_count
    share = mode_total // atom_count
    levels = atom_count // 2
    parity = atom_rank % 2
    level = atom_rank // 2
    extra_rows = (REACH - local_blocks) * block_width
    groups = own_modes // (2 * share)
    split = groups == 1

    low = shifted(eigvec, "atoms", 1)
    high = shifted(eigvec, "atoms", -1)
    far_low = shifted(eigvec[slab_rows - extra_rows :], "atoms", 2)
    far_high = shifted(eigvec[:extra_rows], "atoms", -2)
    eig_half = parity_columns(eigvec, parity, share)
    eig_half_x = swapped(eig_half, "modes", 2)
    eig_pair = jnp.concatenate([eig_half, eig_half_x], axis=0)
    eig_pair_core = swapped(eig_pair, "modes", 1)
    left_eig = eigvec.T

    row_index = lax.dynamic_slice_in_dim(mode_index, mode_rank * own_modes, own_modes)
    col_index = lax.dynamic_slice_in_dim(mode_index, atom_rank * share, share)
    row_freq = looked_up(spectrum, row_index)
    col_freq = looked_up(spectrum, col_index)
    row_width = lax.dynamic_slice_in_dim(linewidth, mode_rank * own_modes, own_modes)
    col_width = lax.dynamic_slice_in_dim(linewidth, atom_rank * share, share)
    offsets = (column_blocks - atom_rank * local_blocks + REACH) % total_blocks

    (offsets, eig_half_x, eig_pair_core, left_eig, row_freq, col_freq, row_width, col_width) = (
        lax.optimization_barrier(
            (offsets, eig_half_x, eig_pair_core, left_eig, row_freq, col_freq, row_width, col_width)
        )
    )

    ext_rows = slab_rows + 2 * REACH * block_width
    full = jax.ShapeDtypeStruct((slab_rows, own_modes), jnp.bfloat16)
    half = jax.ShapeDtypeStruct((slab_rows, own_modes // 2), jnp.bfloat16)
    halves = jax.ShapeDtypeStruct((2 * slab_rows, own_modes // 2), jnp.bfloat16)
    results = pl.pallas_call(
        velocity_kernel(local_blocks, slots, block_width, share, split),
        out_shape=[full, full] + [half, halves] * split,
        in_specs=[in_smem()] * 3 + [in_vmem()] * 6,
        out_specs=[in_vmem()] * (4 if split else 2),
        scratch_shapes=[
            pltpu.VMEM((ext_rows, own_modes), jnp.bfloat16),
            pltpu.VMEM((slots * block_width, own_modes), jnp.bfloat16),
            pltpu.VMEM((block_width, slots * block_width), jnp.bfloat16),
        ],
        name="velocity",
    )(offsets, block_mask, parity[None], far_low, low, eigvec, high, far_high, operator_blocks)
    if split:
        velocity, eig_other, vel_away, mixed = results
    else:
        velocity, eig_other = results
        vel_away = parity_columns(velocity, 1 - parity, share)
        mixed = jnp.concatenate(
            [parity_columns(eig_other, parity, share), parity_columns(velocity, parity, share)],
            axis=0,
        )

    vel_other = swapped(velocity, "atoms", 1)
    vel_other_half_x = swapped_both(vel_away, 1, 2)
    mixed_x = swapped(mixed, "modes", 2)
    mixed_core = swapped(mixed, "modes", 1)
    vel_other_half = parity_columns(vel_other, parity, share)
    vel_other_half_core = swapped(vel_other_half, "modes", 1)
    mixed_far = swapped(mixed_x, "modes", 1)
    vel_other_half_far = swapped(vel_other_half_x, "modes", 1)

    def parts(eig_rows, mixed_rows, vel_rows):
        return (eig_rows, mixed_rows[:slab_rows], mixed_rows[slab_rows:], vel_rows)

    sources = (
        parts(eig_half, mixed, vel_other_half)
        + parts(eig_pair_core[:slab_rows], mixed_core, vel_other_half_core)
        + parts(eig_half_x, mixed_x, vel_other_half_x)
        + parts(eig_pair_core[slab_rows:], mixed_far, vel_other_half_far)
    )
    lefts = (left_eig, eig_other.T, velocity.T, vel_other.T)

    def tile(pick, dtype):
        return pl.pallas_call(
            tile_kernel(4),
            out_shape=jax.ShapeDtypeStruct((own_modes, own_modes // 2), dtype),
            in_specs=[in_smem()] + [in_vmem()] * (4 + len(sources)),
            out_specs=in_vmem(),
            scratch_shapes=[pltpu.VMEM((4 * slab_rows, own_modes // 2), jnp.bfloat16)],
            name="tile",
        )(pick[None], *lefts, *sources)

    if split:

        def tile_for(target, dtype):
            return tile(target ^ mode_rank, dtype)
    else:
        tiles = jnp.stack([tile(jnp.int32(k), jnp.float32) for k in range(mode_count)])

        def tile_for(target, dtype):
            nearness = (target // groups) ^ mode_rank
            start = (nearness, 0, (target % groups) * share)
            return lax.dynamic_slice(tiles, start, (1, own_modes, share))[0].astype(dtype)

    steps = sorted(range(1, levels), key=lambda s: (s not in (2, 3), s))
    arrived = [
        swapped(tile_for(level ^ step, jnp.bfloat16), "atoms", 2 * step) for step in steps
    ]
    flux_tiles = tile_for(level, jnp.float32)
    for piece in arrived:
        flux_tiles = flux_tiles + piece.astype(jnp.float32)

    weight = pair_weight(row_freq, col_freq, row_width, col_width)
    sums = jnp.sum(weight * flux_tiles * flux_tiles, axis=1)
    bit = 1
    while bit < atom_count:
        sums = sums + swapped(sums, "atoms", bit)
        bit *= 2
    return (flux_tiles, sums / mode_total)


def solution(mesh):
    return jax.shard_map(
        body,
        mesh=mesh,
        in_specs=(
            P("atoms", "modes"),
            P("atoms", None, None, None),
            P("atoms", None),
            P("atoms", None),
            P(),
            P(),
            P(),
        ),
        out_specs=(P("modes", "atoms"), P("modes")),
        check_vma=False,
    )
```

```python
import jax
import jax.numpy as jnp
from jax import lax
from jax.experimental import pallas as pl
from jax.experimental.pallas import tpu as pltpu
from jax.sharding import PartitionSpec as P

REACH = 4


def shifted(value, axis, by):
    count = lax.axis_size(axis)
    return lax.ppermute(value, axis, [(i, (i + by) % count) for i in range(count)])


def swapped(value, axis, bit):
    count = lax.axis_size(axis)
    return lax.ppermute(value, axis, [(i, i ^ bit) for i in range(count)])


def swapped_both(value, atom_bit, mode_bit):
    atoms, modes = lax.axis_size("atoms"), lax.axis_size("modes")
    pairs = [
        (a * modes + m, (a ^ atom_bit) * modes + (m ^ mode_bit))
        for a in range(atoms)
        for m in range(modes)
    ]
    return lax.ppermute(value, ("atoms", "modes"), pairs)


def parity_columns(value, parity, share):
    rows, cols = value.shape
    groups = cols // (2 * share)
    if groups == 1:
        return lax.dynamic_slice_in_dim(value, parity * share, share, axis=1)
    split = value.reshape(rows, groups, 2, share)
    return lax.dynamic_index_in_dim(split, parity, 2, keepdims=False).reshape(rows, groups * share)


def looked_up(table, index):
    hit = index[:, None] == jnp.arange(table.shape[0], dtype=index.dtype)[None, :]
    return jnp.sum(jnp.where(hit, table[None, :], 0.0), axis=1)


def pair_weight(row_freq, col_freq, row_width, col_width):
    freq_sum = row_freq[:, None] + col_freq[None, :]
    spacing = row_freq[:, None] - col_freq[None, :]
    mean_width = 0.5 * (row_width[:, None] + col_width[None, :])
    factor = freq_sum * freq_sum / (4.0 * row_freq[:, None] * col_freq[None, :])
    return factor * mean_width / (spacing * spacing + mean_width * mean_width)


def velocity_kernel(local_blocks, slots, block_width, share, split):
    slab_rows = local_blocks * block_width
    base = REACH * block_width

    def kernel(offset, parity, ext, blocks, *rest):
        if split:
            velocity, other, away, mixed, picked = rest
        else:
            velocity, other, picked = rest
        for b in range(local_blocks):
            for s in range(slots):
                source = pl.multiple_of(offset[b, s] * block_width, block_width)
                picked[s * block_width : (s + 1) * block_width, :] = ext[pl.ds(source, block_width), :]
            product = jnp.dot(blocks[b], picked[...], preferred_element_type=jnp.float32)
            velocity[b * block_width : (b + 1) * block_width, :] = product.astype(jnp.bfloat16)
        even = parity[0] == 0
        shift = jnp.where(even, base + slab_rows, base - slab_rows)
        other_rows = ext[pl.ds(pl.multiple_of(shift, block_width), slab_rows), :]
        other[...] = other_rows
        if split:
            mixed[:slab_rows, :] = jnp.where(even, other_rows[:, :share], other_rows[:, share:])
            left, right = velocity[:, :share], velocity[:, share:]
            mixed[slab_rows:, :] = jnp.where(even, left, right)
            away[...] = jnp.where(even, right, left)

    return kernel


def tile_kernel(picks, left, rights, *outs):
    chunks = len(outs) // picks.shape[0]
    turned = left[...].T
    for index in range(picks.shape[0]):
        product = jnp.dot(turned, rights[picks[index]], preferred_element_type=jnp.float32)
        row = 0
        for out in outs[index * chunks : (index + 1) * chunks]:
            out[...] = product[row : row + out.shape[0]].astype(out.dtype)
            row += out.shape[0]


def in_vmem():
    return pl.BlockSpec(memory_space=pltpu.VMEM)


def on_chip(*arrays):
    return tuple(pltpu.with_memory_space_constraint(array, pltpu.VMEM) for array in arrays)


def in_smem():
    return pl.BlockSpec(memory_space=pltpu.SMEM)


def body(eigvec, operator_blocks, column_blocks, block_mask, spectrum, mode_index, linewidth):
    local_blocks, slots, block_width, _ = operator_blocks.shape
    slab_rows, own_modes = eigvec.shape
    atom_count = lax.axis_size("atoms")
    mode_count = lax.axis_size("modes")
    atom_rank = lax.axis_index("atoms")
    mode_rank = lax.axis_index("modes")
    total_blocks = local_blocks * atom_count
    mode_total = own_modes * mode_count
    share = mode_total // atom_count
    levels = atom_count // 2
    parity = atom_rank % 2
    level = atom_rank // 2
    extra_rows = (REACH - local_blocks) * block_width
    groups = own_modes // (2 * share)
    split = groups == 1

    low = shifted(eigvec, "atoms", 1)
    high = shifted(eigvec, "atoms", -1)
    far_low = shifted(eigvec[slab_rows - extra_rows :], "atoms", 2)
    far_high = shifted(eigvec[:extra_rows], "atoms", -2)
    eig_half = parity_columns(eigvec, parity, share)
    eig_half_x = swapped(eig_half, "modes", 2)

    row_index = lax.dynamic_slice_in_dim(mode_index, mode_rank * own_modes, own_modes)
    col_index = lax.dynamic_slice_in_dim(mode_index, atom_rank * share, share)
    row_freq = looked_up(spectrum, row_index)
    col_freq = looked_up(spectrum, col_index)
    row_width = lax.dynamic_slice_in_dim(linewidth, mode_rank * own_modes, own_modes)
    col_width = lax.dynamic_slice_in_dim(linewidth, atom_rank * share, share)
    offsets = (column_blocks - atom_rank * local_blocks + REACH) % total_blocks

    masked = jnp.where(
        block_mask[:, :, None, None] > 0, operator_blocks, jnp.zeros((), operator_blocks.dtype)
    )
    masked = masked.transpose(0, 2, 1, 3).reshape(local_blocks, block_width, slots * block_width)
    (offsets, masked, eig_half_x, row_freq, col_freq, row_width, col_width) = (
        lax.optimization_barrier(
            (offsets, masked, eig_half_x, row_freq, col_freq, row_width, col_width)
        )
    )

    extended = jnp.concatenate([far_low, low, eigvec, high, far_high], axis=0)
    full = pltpu.VMEM((slab_rows, own_modes), jnp.bfloat16)
    half = pltpu.VMEM((slab_rows, own_modes // 2), jnp.bfloat16)
    halves = pltpu.VMEM((2 * slab_rows, own_modes // 2), jnp.bfloat16)
    results = pl.pallas_call(
        velocity_kernel(local_blocks, slots, block_width, share, split),
        out_shape=[full, full] + [half, halves] * split,
        in_specs=[in_smem()] * 2 + [in_vmem()] * 2,
        out_specs=[in_vmem()] * (4 if split else 2),
        scratch_shapes=[
            pltpu.VMEM((slots * block_width, own_modes), jnp.bfloat16),
        ],
        compiler_params=pltpu.CompilerParams(vmem_limit_bytes=8 << 20),
        name="velocity",
    )(offsets, parity[None], *on_chip(extended, masked))
    if split:
        velocity, eig_other, vel_away, mixed = results
    else:
        velocity, eig_other = results
        vel_away = parity_columns(velocity, 1 - parity, share)
        mixed = jnp.concatenate(
            [parity_columns(eig_other, parity, share), parity_columns(velocity, parity, share)],
            axis=0,
        )

    eig_pair_core = swapped(jnp.concatenate([eig_half, eig_half_x], axis=0), "modes", 1)
    vel_other = swapped(velocity, "atoms", 1)
    vel_other_half_x = swapped_both(vel_away, 1, 2)
    mixed_x = swapped(mixed, "modes", 2)
    mixed_core = swapped(mixed, "modes", 1)
    vel_other_half = parity_columns(vel_other, parity, share)
    vel_other_half_core = swapped(vel_other_half, "modes", 1)
    mixed_far = swapped(mixed_x, "modes", 1)
    vel_other_half_far = swapped(vel_other_half_x, "modes", 1)

    def stacked(eig_rows, mixed_rows, vel_rows):
        return jnp.concatenate(
            [mixed_rows[slab_rows:], vel_rows, -eig_rows, -mixed_rows[:slab_rows]], axis=0
        )

    rights = jnp.stack(
        [
            stacked(eig_half, mixed, vel_other_half),
            stacked(eig_pair_core[:slab_rows], mixed_core, vel_other_half_core),
            stacked(eig_half_x, mixed_x, vel_other_half_x),
            stacked(eig_pair_core[slab_rows:], mixed_far, vel_other_half_far),
        ]
    )
    width = own_modes // 2

    def tiles_of(picks, dtypes, heights, *after):
        lefts = (eigvec, eig_other, velocity, vel_other)
        picks, *rest = lax.optimization_barrier((picks, *lefts, *after))
        left = jnp.concatenate(rest[: len(lefts)], axis=0)
        outs = [pltpu.VMEM((rows, width), dtype) for dtype in dtypes for rows in heights]
        found = pl.pallas_call(
            tile_kernel,
            out_shape=outs,
            in_specs=[in_smem()] + [in_vmem()] * 2,
            out_specs=[in_vmem()] * len(outs),
            compiler_params=pltpu.CompilerParams(vmem_limit_bytes=8 << 20),
            name="tile",
        )(picks, *on_chip(left, rights))
        chunks = len(heights)
        return [list(found[i : i + chunks]) for i in range(0, len(found), chunks)]

    order = sorted(range(levels), key=lambda d: (-(d & 1), -d))
    if split:
        heights = (width, width)
        picks = jnp.stack([level ^ d ^ mode_rank for d in order])
        dtypes = [jnp.bfloat16 if d & 1 else jnp.float32 for d in order]
        first = tiles_of(picks[:1], dtypes[:1], heights)
        others = tiles_of(picks[1:], dtypes[1:], heights, *first[0])
        held = dict(zip(order, first + others))
    else:
        picks = jnp.arange(mode_count, dtype=jnp.int32)
        dtypes = [jnp.float32] * mode_count
        every = jnp.stack([t[0] for t in tiles_of(picks, dtypes, (own_modes,))])
        held = {}
        for d in order:
            target = level ^ d
            start = ((target // groups) ^ mode_rank, 0, (target % groups) * share)
            held[d] = [lax.dynamic_slice(every, start, (1, own_modes, share))[0]]

    bit = 1
    while bit < levels:
        for distance in sorted((d for d in held if d & bit), reverse=True):
            pieces = held.pop(distance)
            for index, piece in enumerate(pieces):
                if distance == bit and bit * 2 in held and split:
                    piece, _ = lax.optimization_barrier((piece, held[bit * 2][index]))
                got = swapped(piece.astype(jnp.bfloat16), "atoms", 2 * bit)
                kept = held[distance ^ bit]
                kept[index] = kept[index] + got.astype(jnp.float32)
        bit *= 2
    tiles = held[0]

    sums = []
    row = 0
    for part in tiles:
        rows = slice(row, row + part.shape[0])
        row += part.shape[0]
        weight = pair_weight(row_freq[rows], col_freq, row_width[rows], col_width)
        sums.append(jnp.sum(weight * part * part, axis=1))
    sums = jnp.concatenate(sums)
    sums = sums + swapped(sums, "atoms", 1)
    if levels <= 4:
        others = [swapped(sums, "atoms", 2 * step) for step in (2, 3, 1) if step < levels]
        sums = sums + sum(others)
    else:
        bit = 2
        while bit < atom_count:
            sums = sums + swapped(sums, "atoms", bit)
            bit *= 2
    return (jnp.concatenate(tiles, axis=0), sums / mode_total)


def solution(mesh):
    return jax.shard_map(
        body,
        mesh=mesh,
        in_specs=(
            P("atoms", "modes"),
            P("atoms", None, None, None),
            P("atoms", None),
            P("atoms", None),
            P(),
            P(),
            P(),
        ),
        out_specs=(P("modes", "atoms"), P("modes")),
        check_vma=False,
    )
```

```python
import jax
import jax.numpy as jnp
from jax import lax
from jax.experimental import pallas as pl
from jax.experimental.pallas import tpu as pltpu
from jax.sharding import PartitionSpec as P


REACH = 4


def shifted(value, axis, by):
    count = lax.axis_size(axis)
    return lax.ppermute(value, axis, [(i, (i + by) % count) for i in range(count)])


def swapped(value, axis, bit):
    count = lax.axis_size(axis)
    return lax.ppermute(value, axis, [(i, i ^ bit) for i in range(count)])


def swapped_both(value, atom_bit, mode_bit):
    atoms, modes = lax.axis_size("atoms"), lax.axis_size("modes")
    pairs = [
        (a * modes + m, (a ^ atom_bit) * modes + (m ^ mode_bit))
        for a in range(atoms)
        for m in range(modes)
    ]
    return lax.ppermute(value, ("atoms", "modes"), pairs)


def parity_columns(value, parity, share):
    rows, cols = value.shape
    groups = cols // (2 * share)
    if groups == 1:
        return lax.dynamic_slice_in_dim(value, parity * share, share, axis=1)
    split = value.reshape(rows, groups, 2, share)
    return lax.dynamic_index_in_dim(split, parity, 2, keepdims=False).reshape(rows, groups * share)


def merged(at_parity, elsewhere, parity, share):
    rows, cols = at_parity.shape
    if cols == share:
        even = jnp.concatenate([at_parity, elsewhere], axis=1)
        odd = jnp.concatenate([elsewhere, at_parity], axis=1)
    else:
        here = at_parity.reshape(rows, -1, 1, share)
        there = elsewhere.reshape(rows, -1, 1, share)
        even = jnp.concatenate([here, there], axis=2).reshape(rows, -1)
        odd = jnp.concatenate([there, here], axis=2).reshape(rows, -1)
    return jnp.where(parity == 0, even, odd)


def looked_up(table, index):
    hit = index[:, None] == jnp.arange(table.shape[0], dtype=index.dtype)[None, :]
    return jnp.sum(jnp.where(hit, table[None, :], 0.0), axis=1)


def pair_weight(row_freq, col_freq, row_width, col_width):
    freq_sum = row_freq[:, None] + col_freq[None, :]
    spacing = row_freq[:, None] - col_freq[None, :]
    mean_width = 0.5 * (row_width[:, None] + col_width[None, :])
    factor = freq_sum * freq_sum / (4.0 * row_freq[:, None] * col_freq[None, :])
    return factor * mean_width / (spacing * spacing + mean_width * mean_width)


def velocity_kernel(local_blocks, slots, block_width, share, split):
    slab_rows = local_blocks * block_width
    base = (2 * REACH - local_blocks) * block_width

    def kernel(offset, parity, ext, blocks, *rest):
        if split:
            velocity, other, away, mixed, picked = rest
        else:
            velocity, other, picked = rest
        for b in range(local_blocks):
            for s in range(slots):
                source = pl.multiple_of(offset[b, s] * block_width, block_width)
                picked[s * block_width : (s + 1) * block_width, :] = ext[pl.ds(source, block_width), :]
            product = jnp.dot(blocks[b], picked[...], preferred_element_type=jnp.float32)
            velocity[b * block_width : (b + 1) * block_width, :] = product.astype(jnp.bfloat16)
        even = parity[0] == 0
        shift = jnp.where(even, base + slab_rows, base - slab_rows)
        other_rows = ext[pl.ds(pl.multiple_of(shift, block_width), slab_rows), :]
        other[...] = other_rows
        if split:
            mixed[:slab_rows, :] = jnp.where(even, other_rows[:, :share], other_rows[:, share:])
            left, right = velocity[:, :share], velocity[:, share:]
            mixed[slab_rows:, :] = jnp.where(even, left, right)
            away[...] = jnp.where(even, right, left)

    return kernel


def tile_kernel(picks, left, rights, *outs):
    chunks = len(outs) // picks.shape[0]
    turned = left[...].T
    for index in range(picks.shape[0]):
        product = jnp.dot(turned, rights[picks[index]], preferred_element_type=jnp.float32)
        row = 0
        for out in outs[index * chunks : (index + 1) * chunks]:
            out[...] = product[row : row + out.shape[0]].astype(out.dtype)
            row += out.shape[0]


def in_vmem():
    return pl.BlockSpec(memory_space=pltpu.VMEM)


def on_chip(*arrays):
    return tuple(pltpu.with_memory_space_constraint(array, pltpu.VMEM) for array in arrays)


def in_smem():
    return pl.BlockSpec(memory_space=pltpu.SMEM)


def body(eigvec, operator_blocks, column_blocks, block_mask, spectrum, mode_index, linewidth):
    local_blocks, slots, block_width, _ = operator_blocks.shape
    slab_rows, own_modes = eigvec.shape
    atom_count = lax.axis_size("atoms")
    mode_count = lax.axis_size("modes")
    atom_rank = lax.axis_index("atoms")
    mode_rank = lax.axis_index("modes")
    total_blocks = local_blocks * atom_count
    mode_total = own_modes * mode_count
    share = mode_total // atom_count
    levels = atom_count // 2
    parity = atom_rank % 2
    level = atom_rank // 2
    extra_rows = (REACH - local_blocks) * block_width
    groups = own_modes // (2 * share)
    split = groups == 1

    low = shifted(eigvec, "atoms", 1)
    high = shifted(eigvec, "atoms", -1)
    far_low = shifted(eigvec[slab_rows - extra_rows :], "atoms", 2)
    far_high = shifted(eigvec[:extra_rows], "atoms", -2)
    eig_half = parity_columns(eigvec, parity, share)
    eig_half_x = swapped(eig_half, "modes", 2)

    offsets = (column_blocks - atom_rank * local_blocks + REACH) % total_blocks
    extra = REACH - local_blocks
    offsets = jnp.where(
        offsets < extra,
        offsets,
        jnp.where(
            offsets < extra + 3 * local_blocks, offsets + extra, offsets - 3 * local_blocks
        ),
    )

    masked = jnp.where(
        block_mask[:, :, None, None] > 0, operator_blocks, jnp.zeros((), operator_blocks.dtype)
    )
    masked = masked.transpose(0, 2, 1, 3).reshape(local_blocks, block_width, slots * block_width)
    offsets, masked, eig_half_x = lax.optimization_barrier((offsets, masked, eig_half_x))

    ends = lax.optimization_barrier(jnp.concatenate([far_low, far_high], axis=0))
    extended = jnp.concatenate([ends, low, eigvec, high], axis=0)
    full = pltpu.VMEM((slab_rows, own_modes), jnp.bfloat16)
    half = pltpu.VMEM((slab_rows, own_modes // 2), jnp.bfloat16)
    halves = pltpu.VMEM((2 * slab_rows, own_modes // 2), jnp.bfloat16)
    results = pl.pallas_call(
        velocity_kernel(local_blocks, slots, block_width, share, split),
        out_shape=[full, full] + [half, halves] * split,
        in_specs=[in_smem()] * 2 + [in_vmem()] * 2,
        out_specs=[in_vmem()] * (4 if split else 2),
        scratch_shapes=[
            pltpu.VMEM((slots * block_width, own_modes), jnp.bfloat16),
        ],
        compiler_params=pltpu.CompilerParams(vmem_limit_bytes=8 << 20),
        name="velocity",
    )(offsets, parity[None], *on_chip(extended, masked))
    if split:
        velocity, eig_other, vel_away, mixed = results
    else:
        velocity, eig_other = results
        vel_away = parity_columns(velocity, 1 - parity, share)
        mixed = jnp.concatenate(
            [parity_columns(eig_other, parity, share), parity_columns(velocity, parity, share)],
            axis=0,
        )

    spectrum, mode_index, linewidth, velocity = lax.optimization_barrier(
        (spectrum, mode_index, linewidth, velocity)
    )
    row_index = lax.dynamic_slice_in_dim(mode_index, mode_rank * own_modes, own_modes)
    col_index = lax.dynamic_slice_in_dim(mode_index, atom_rank * share, share)
    row_freq = looked_up(spectrum, row_index)
    col_freq = looked_up(spectrum, col_index)
    row_width = lax.dynamic_slice_in_dim(linewidth, mode_rank * own_modes, own_modes)
    col_width = lax.dynamic_slice_in_dim(linewidth, atom_rank * share, share)

    eig_pair_core = swapped(jnp.concatenate([eig_half, eig_half_x], axis=0), "modes", 1)
    mixed_x = swapped(mixed, "modes", 2)
    vel_other_half = swapped(vel_away, "atoms", 1)
    vel_other_rest = swapped(mixed[slab_rows:], "atoms", 1)
    vel_other_half_x = swapped_both(vel_away, 1, 2)
    mixed_core = swapped(mixed, "modes", 1)
    vel_other_half_core = swapped(vel_other_half, "modes", 1)
    mixed_far = swapped(mixed_x, "modes", 1)
    vel_other_half_far = swapped(vel_other_half_x, "modes", 1)
    vel_other = lax.optimization_barrier(merged(vel_other_half, vel_other_rest, parity, share))
    flipped = lax.optimization_barrier(-mixed[:slab_rows])

    def stacked(eig_rows, mixed_rows, vel_rows, minus=None):
        minus = -mixed_rows[:slab_rows] if minus is None else minus
        return jnp.concatenate([mixed_rows[slab_rows:], vel_rows, -eig_rows, minus], axis=0)

    rights = jnp.stack(
        [
            stacked(eig_half, mixed, vel_other_half, flipped),
            stacked(eig_pair_core[:slab_rows], mixed_core, vel_other_half_core),
            stacked(eig_half_x, mixed_x, vel_other_half_x),
            stacked(eig_pair_core[slab_rows:], mixed_far, vel_other_half_far),
        ]
    )
    width = own_modes // 2

    def tiles_of(picks, dtypes, heights, *after):
        lefts = (eigvec, eig_other, velocity, vel_other)
        picks, *rest = lax.optimization_barrier((picks, *lefts, *after))
        left = jnp.concatenate(rest[: len(lefts)], axis=0)
        outs = [pltpu.VMEM((rows, width), dtype) for dtype in dtypes for rows in heights]
        found = pl.pallas_call(
            tile_kernel,
            out_shape=outs,
            in_specs=[in_smem()] + [in_vmem()] * 2,
            out_specs=[in_vmem()] * len(outs),
            compiler_params=pltpu.CompilerParams(vmem_limit_bytes=8 << 20),
            name="tile",
        )(picks, *on_chip(left, rights))
        chunks = len(heights)
        return [list(found[i : i + chunks]) for i in range(0, len(found), chunks)]

    order = sorted(range(levels), key=lambda d: (-(d & 1), -d))
    if split:
        heights = (width, width)
        picks = jnp.stack([level ^ d ^ mode_rank for d in order])
        dtypes = [jnp.bfloat16 if d & 1 else jnp.float32 for d in order]
        first = tiles_of(picks[:1], dtypes[:1], heights)
        others = tiles_of(picks[1:], dtypes[1:], heights, *first[0])
        held = dict(zip(order, first + others))
    else:
        picks = jnp.arange(mode_count, dtype=jnp.int32)
        dtypes = [jnp.float32] * mode_count
        every = jnp.stack([t[0] for t in tiles_of(picks, dtypes, (own_modes,))])
        held = {}
        for d in order:
            target = level ^ d
            start = ((target // groups) ^ mode_rank, 0, (target % groups) * share)
            held[d] = [lax.dynamic_slice(every, start, (1, own_modes, share))[0]]

    bit = 1
    while bit < levels:
        for distance in sorted((d for d in held if d & bit), reverse=True):
            pieces = held.pop(distance)
            for index, piece in enumerate(pieces):
                if distance == bit and bit * 2 in held and split:
                    piece, _ = lax.optimization_barrier((piece, held[bit * 2][index]))
                got = swapped(piece.astype(jnp.bfloat16), "atoms", 2 * bit)
                kept = held[distance ^ bit]
                kept[index] = kept[index] + got.astype(jnp.float32)
        bit *= 2
    tiles = held[0]

    sums = []
    row = 0
    for part in tiles:
        rows = slice(row, row + part.shape[0])
        row += part.shape[0]
        weight = pair_weight(row_freq[rows], col_freq, row_width[rows], col_width)
        sums.append(jnp.sum(weight * part * part, axis=1))
    sums = jnp.concatenate(sums)
    if levels <= 4:
        others = [swapped(sums, "atoms", 2 * step) for step in (2, 3, 1) if step < levels]
        sums = sums + sum(others)
    else:
        bit = 2
        while bit < atom_count:
            sums = sums + swapped(sums, "atoms", bit)
            bit *= 2
    sums = sums + swapped(sums, "atoms", 1)
    return (jnp.concatenate(tiles, axis=0), sums / mode_total)


def solution(mesh):
    return jax.shard_map(
        body,
        mesh=mesh,
        in_specs=(
            P("atoms", "modes"),
            P("atoms", None, None, None),
            P("atoms", None),
            P("atoms", None),
            P(),
            P(),
            P(),
        ),
        out_specs=(P("modes", "atoms"), P("modes")),
        check_vma=False,
    )
```
